32 devices in a mesh: groups: 2 (over y), rows: 4 (over z), cols: 2 (over x), sub: 2 (over core).
Axes of the slice: x: 2, y: 2, z: 4, core: 2. Of those that a mesh axis runs over, the one named last changes fastest.
Arguments:
- stored_vectors: bfloat16 [3072, 8192], P(('cols', 'sub'), ('groups', 'rows')), parts along dimension 1, may hold values from -0.59765625 to 0.59765625
- previous_columns: bfloat16 [8192, 256], P(('groups', 'rows', 'cols', 'sub')), parts along dimension 0, may hold values from -3 to 3
- pivots: int32 [512], P('groups'), parts along dimension 0, may hold values from 0 to 4095, as said below
- diagonal: float32 [8192], P(('groups', 'rows', 'cols', 'sub')), parts along dimension 0, may hold values from 2 to 32
- ket_blocks: bfloat16 [128, 128, 256], P(('groups', 'rows', 'cols', 'sub')), parts along dimension 0, may hold values from -6 to 6
- shell_tags: int32 [128, 128], P(('groups', 'rows', 'cols', 'sub')), parts along dimension 0, may hold values from 0 to 3
- target_blocks: int32 [32, 4], P('groups'), parts along dimension 0, may hold values from 0 to 31, as said below
- block_counts: int32 [32], P('groups'), parts along dimension 0, may hold values from 0 to 4, as said below
- shell_norms: float32 [4], replicated, may hold values from 0.5 to 2
Outputs:
- new_vectors: bfloat16 [8192, 256], P(('groups', 'rows', 'cols', 'sub')), parts along dimension 0
- diag_out: float32 [8192], P(('groups', 'rows', 'cols', 'sub')), parts along dimension 0
- next_columns: bfloat16 [8192, 256], P(('groups', 'rows', 'cols', 'sub')), parts along dimension 0
The draws below stay inside these ranges and needn't reach their ends.
There are 2 independent parts, one for each index of `groups`. The reference program is written for one: setup_inputs(seed, part) draws one part's arguments, and reference() takes and returns one part's arrays. A program takes and returns all parts, laid end to end along the dimension named above; an argument that names none is the same for every part. Nothing has to cross between parts.
Inputs may be any that keep to these rules, and one draw needn't show every extreme that they name: `pivots`: 256 distinct AO pairs. `target_blocks`: the used slots of all owners name every block of the 32 blocks exactly once; a used slot's block lies on a device with the owner's cols and sub indices (blocks g * 2 to g * 2 + 1 lie on the device of linear index g, rows slowest; owner o is the device of linear index o). At most 1 of one owner's used slots go to one device, and some owner reaches that in every draw. Entries of unused slots are arbitrary blocks. `block_counts`: some owner uses all 4 slots in every draw.
All inputs are finite; a program needn't handle non-finite values.
Results may differ from the reference program's by a relative error of at most 0.0004.
Values may be sent and summed in bfloat16 or wider, within the bound.
A program may use at most 64 MiB of HBM per device.

```python
import math
import jax
import jax.numpy as jnp
from jax import lax

K = 3072
B = 256
BLK = 128
BLOCKS_DEV = 2
SHELL_TYPES = 4
CAP = 4
OWNERS = 16
PAIRS = 4096
N_ROWS = 4
N_COLS = 2
N_SUB = 2


def layout_draw(key):
    band_count = N_ROWS
    column = N_COLS * N_SUB
    per_device = BLOCKS_DEV
    slot_count = 2 * BLOCKS_DEV
    base = jax.random.fold_in(key, 11)
    keys = jax.random.split(base, 4)
    ranks = jnp.arange(band_count, dtype=jnp.int32)
    rank_counts = jnp.where(ranks == 0, slot_count, jnp.where(ranks == 1, 0, per_device)).astype(jnp.int32)
    rank_starts = (jnp.cumsum(rank_counts) - rank_counts).astype(jnp.int32)
    order = jax.vmap(lambda sub_key: jax.random.permutation(sub_key, band_count))(jax.random.split(keys[0], column)).astype(jnp.int32)
    lines = jnp.arange(column, dtype=jnp.int32)[:, None]
    counts = jnp.zeros((column, band_count), jnp.int32).at[lines, order].set(jnp.broadcast_to(rank_counts, (column, band_count)))
    starts = jnp.zeros((column, band_count), jnp.int32).at[lines, order].set(jnp.broadcast_to(rank_starts, (column, band_count)))
    total = band_count * per_device
    receiver_order = jax.vmap(lambda sub_key: jax.random.permutation(sub_key, band_count))(jax.random.split(keys[1], column)).astype(jnp.int32)
    within_order = jax.vmap(lambda sub_key: jax.random.permutation(sub_key, per_device))(jax.random.split(keys[2], column)).astype(jnp.int32)
    slots = jnp.arange(slot_count, dtype=jnp.int32)
    position = jnp.minimum(starts[:, :, None] + slots[None, None, :], total - 1)
    receiver_spread = jnp.broadcast_to(receiver_order[:, None, :], (column, band_count, band_count))
    receiver = jnp.take_along_axis(receiver_spread, position % band_count, axis=2)
    within_spread = jnp.broadcast_to(within_order[:, None, :], (column, band_count, per_device))
    within = jnp.take_along_axis(within_spread, position // band_count, axis=2)
    target = (receiver * column + jnp.arange(column, dtype=jnp.int32)[:, None, None]) * per_device + within
    filler = jax.random.randint(keys[3], (column, band_count, slot_count), 0, band_count * column * per_device).astype(jnp.int32)
    valid = slots[None, None, :] < counts[:, :, None]
    target = jnp.where(valid, target, filler)
    target = jnp.transpose(target, (1, 0, 2)).reshape(band_count * column, slot_count)
    owner_counts = jnp.transpose(counts, (1, 0)).reshape(band_count * column)
    return (target.astype(jnp.int32), owner_counts.astype(jnp.int32))


def draw_target_blocks(key, part):
    return layout_draw(key)[0]


def draw_block_counts(key, part):
    return layout_draw(key)[1]


def draw_pivots(key, part):
    chosen = jax.random.permutation(jax.random.fold_in(key, 5), PAIRS)
    return chosen[:B].astype(jnp.int32)


def place_ends(entries, key, smallest, largest):
    longest = entries.shape.index(max(entries.shape))
    spots = []
    for shift in (0, 1):
        where = [jax.random.randint(jax.random.fold_in(key, axis), (), 0, length) for axis, length in enumerate(entries.shape)]
        where[longest] = (where[longest] + shift) % entries.shape[longest]
        spots.append(tuple(where))
    return entries.at[spots[0]].set(smallest).at[spots[1]].set(largest)


def block_levels(rng, extent, cuts, low, high):
    gain = 1.0
    for dim, shards_of in cuts:
        draws = jax.random.uniform(jax.random.fold_in(jax.random.fold_in(rng, 6), dim), (shards_of,), jnp.float32, low / len(cuts), high / len(cuts))
        gain = gain * jnp.repeat(jnp.exp(draws), extent[dim] // shards_of).reshape((-1,) + (1,) * (len(extent) - 1 - dim))
    return gain


def centred(own_key, extent, scale, most, pieces=(), kind=jnp.bfloat16):
    entries = scale * jax.random.normal(own_key, extent, jnp.float32)
    if pieces:
        entries = entries * block_levels(own_key, extent, pieces, -0.22, 0.18)
    return jnp.clip(entries, -most, most).astype(kind)


def setup_inputs(seed: int = 0, part: int = 0) -> dict:
    seeds = jax.random.split(jax.random.key(seed), 10)
    part_keys = jax.random.split(jax.random.fold_in(seeds[9], part), 10)
    return {
        "stored_vectors": centred(part_keys[0], (K, PAIRS), 0.1, 0.59765625, ((0, 4), (1, 4))),
        "previous_columns": centred(part_keys[1], (PAIRS, B), 0.5, 3.0, ((0, 16),)),
        "pivots": draw_pivots(jax.random.fold_in(jax.random.fold_in(seeds[9], part), 71), part),
        "diagonal": jnp.clip(jnp.exp(math.log(32.0) - 2.7725887 * jax.random.uniform(part_keys[3], (PAIRS,), jnp.float32) ** block_levels(part_keys[3], (PAIRS,), ((0, 16),), -0.2, 0.2)), 2.0, 32.0),
        "ket_blocks": centred(part_keys[4], (OWNERS * CAP, BLK, B), 1.0, 6.0, ((0, 16),)),
        "shell_tags": place_ends(jax.random.randint(part_keys[5], (OWNERS * CAP, BLK), 0, SHELL_TYPES), jax.random.fold_in(part_keys[5], 1), 0, SHELL_TYPES - 1).astype(jnp.int32),
        "target_blocks": draw_target_blocks(jax.random.fold_in(jax.random.fold_in(seeds[9], part), 71), part),
        "block_counts": draw_block_counts(jax.random.fold_in(jax.random.fold_in(seeds[9], part), 71), part),
        "shell_norms": jnp.clip(jnp.exp(jax.random.uniform(seeds[8], (SHELL_TYPES,), jnp.float32, math.log(0.5), math.log(2.0))), 0.5, 2.0),
    }


def reference(stored_vectors, previous_columns, pivots, diagonal, ket_blocks, shell_tags, target_blocks, block_counts, shell_norms):
    kinds = jnp.arange(shell_norms.shape[0], dtype=jnp.int32)
    factor = lax.optimization_barrier(jnp.sum(jnp.where(shell_tags[..., None] == kinds, shell_norms, jnp.float32(0.0)), axis=-1))
    fresh = (ket_blocks.astype(jnp.float32) * factor[..., None]).astype(jnp.bfloat16)
    slots = jnp.arange(CAP, dtype=jnp.int32)
    valid = slots[None, :] < block_counts[:, None]
    blocks_total = PAIRS // BLK
    placing = jnp.where(valid, target_blocks, blocks_total).reshape(-1).astype(jnp.int32)
    placed = jnp.zeros((blocks_total, BLK, B), jnp.bfloat16).at[placing].set(fresh, mode='drop')
    next_columns = placed.reshape(PAIRS, B)
    pivot_rows = stored_vectors[:, pivots]
    groups_count = N_COLS * N_SUB
    width = K // groups_count
    product = jnp.zeros((PAIRS, B), jnp.float32)
    for group in range(groups_count):
        block_vectors = stored_vectors[group * width:(group + 1) * width]
        block_pivots = pivot_rows[group * width:(group + 1) * width]
        partial_sum = jnp.dot(block_vectors.T, block_pivots, preferred_element_type=jnp.float32)
        product = product + partial_sum
    residual_cols = previous_columns.astype(jnp.float32) - product
    pivot_diag = diagonal[pivots]
    scaled = residual_cols / jnp.sqrt(pivot_diag)[None, :]
    new_vectors = scaled.astype(jnp.bfloat16)
    diag_out = diagonal - lax.optimization_barrier(jnp.sum(scaled * scaled, axis=1))
    return (new_vectors, diag_out, next_columns)
```

```python
import functools

import jax
import jax.numpy as jnp
from jax import lax
from jax.experimental import pallas as pl
from jax.experimental.pallas import tpu as pltpu
from jax.sharding import PartitionSpec as P

MESH = pl.DeviceIdType.MESH
LANES = 128


def column_of(row):
    return jnp.transpose(jnp.broadcast_to(row, (LANES, row.shape[1])))


def kernel(
    sizes,
    vec_hbm, prev_hbm, piv_ref, diag_ref, ket_hbm, tags_ref, targets_ref, counts_ref, norms_ref,
    new_ref, diag_out_ref, next_ref,
    vec, prev, ket, hot, own, fwd_r, fwd_l, from_l, from_r,
    pivot_t, prev_t, sub_out, sub_in, mine, col_out, col_in, scaled_t,
    stage, landed, pd_z, pd_s, pd_c, pd_own_s, pd_own_c,
    load_sem, zr_send, zl_send, l_recv, r_recv, sub_send, sub_recv, col_send, col_recv,
    ket_send, ket_recv, pdz_send, pdz_recv, pds_send, pds_recv, pdc_send, pdc_recv,
):
    n_rows, n_cols, n_sub, hop_lead = sizes
    z, x, s = lax.axis_index("rows"), lax.axis_index("cols"), lax.axis_index("sub")
    column_size = n_cols * n_sub
    column = x * n_sub + s
    device = z * column_size + column
    slot_count, block_rows, batch = ket_hbm.shape
    rows_here = prev_hbm.shape[0]
    per_device = rows_here // block_rows
    width, band_rows = vec_hbm.shape
    z_chunks, z_rows = own.shape[0], own.shape[1]
    m_chunks, m_rows = mine.shape[0], mine.shape[1]
    per_m = m_rows // z_rows

    load_ket = pltpu.make_async_copy(ket_hbm, ket, load_sem.at[0])
    load_vec = pltpu.make_async_copy(vec_hbm, vec, load_sem.at[1])
    load_prev = pltpu.make_async_copy(prev_hbm, prev, load_sem.at[2])
    load_ket.start()
    load_vec.start()
    load_prev.start()

    barrier = pltpu.get_barrier_semaphore()
    for name, here, count in (("rows", z, n_rows), ("cols", x, n_cols), ("sub", s, n_sub)):
        for d in range(1, count):
            pl.semaphore_signal(
                barrier, inc=1, device_id={name: lax.rem(here + d, count)}, device_id_type=MESH
            )

    piv_col = column_of(piv_ref[...].astype(jnp.float32)).astype(jnp.int32) - z * band_rows
    lane = lax.broadcasted_iota(jnp.int32, (batch, LANES), 1)
    for t in range(band_rows // LANES):
        hot[:, t * LANES:(t + 1) * LANES] = (piv_col == lane + t * LANES).astype(
            jnp.float32).astype(jnp.bfloat16)

    tags = tags_ref[...]
    factor = jnp.zeros(tags.shape, jnp.float32)
    for kind in range(norms_ref.shape[0]):
        factor = jnp.where(tags == kind, norms_ref[kind], factor)
    load_ket.wait()
    for slot in range(slot_count):
        scale = column_of(factor[slot:slot + 1, :])
        for h in range(batch // LANES):
            part = (slot, slice(None), slice(h * LANES, (h + 1) * LANES))
            ket[part] = (ket[part].astype(jnp.float32) * scale).astype(jnp.bfloat16)
    used = counts_ref[device]

    def stage_for(band):
        low = (band * column_size + column) * per_device
        chosen = jnp.int32(0)
        for slot in range(slot_count):
            target = targets_ref[device, slot]
            fits = (slot < used) & (target >= low) & (target < low + per_device)
            chosen = jnp.where(fits, jnp.int32(slot), chosen)
        return ket[chosen]

    landed[z] = stage_for(z)
    for d in range(1, n_rows):
        stage[d] = stage_for(lax.rem(z + d, n_rows))

    def ket_copy(d):
        return pltpu.make_async_remote_copy(
            src_ref=stage.at[d], dst_ref=landed.at[z], send_sem=ket_send.at[d],
            recv_sem=ket_recv.at[z], device_id={"rows": lax.rem(z + d, n_rows)},
            device_id_type=MESH)

    pl.semaphore_wait(barrier, n_rows + n_cols + n_sub - 3)

    def near(d):
        right = z < n_rows - 1 if d == 1 else False
        left = z > 0 if d == n_rows - 1 else False
        return jnp.logical_or(right, left)

    for d in range(1, n_rows):
        @pl.when(jnp.logical_not(near(d)))
        def _():
            ket_copy(d).start()

    def z_copy(src, dst, send, recv, q, dz):
        return pltpu.make_async_remote_copy(
            src_ref=src.at[q], dst_ref=dst.at[q], send_sem=send.at[q], recv_sem=recv.at[q],
            device_id={"rows": lax.rem(z + dz + n_rows, n_rows)}, device_id_type=MESH)

    def arrived(dst, sem):
        pltpu.make_async_remote_copy(
            src_ref=dst, dst_ref=dst, send_sem=sem, recv_sem=sem,
            device_id={"sub": lax.rem(s + 1, n_sub)}, device_id_type=MESH).wait_recv()

    load_vec.wait()
    piece = min(LANES, batch)
    in_piece = piece // z_rows
    for p in range(batch // piece):
        got = lax.dot_general(
            hot[p * piece:(p + 1) * piece, :], vec[...], (((1,), (1,)), ((), ())),
            preferred_element_type=jnp.float32).astype(jnp.bfloat16)
        got = got.reshape(in_piece, z_rows, width)
        own[p * in_piece:(p + 1) * in_piece] = got

        @pl.when(z == 0)
        def _():
            fwd_r[p * in_piece:(p + 1) * in_piece] = got
            for q in range(p * in_piece, (p + 1) * in_piece):
                z_copy(own, from_l, zr_send, l_recv, q, 1).start()

        @pl.when(z == n_rows - 1)
        def _():
            for q in range(p * in_piece, (p + 1) * in_piece):
                z_copy(own, from_r, zl_send, r_recv, q, -1).start()

    diag_col = column_of(diag_ref[...])
    row = lax.broadcasted_iota(jnp.int32, (rows_here, LANES), 0) + device * rows_here
    for h in range(batch // LANES):
        cut = slice(h * LANES, (h + 1) * LANES)
        share = jnp.sum(jnp.where(piv_ref[:, cut] == row, diag_col, 0.0), axis=0, keepdims=True)
        pd_z[n_rows, :, cut] = jnp.broadcast_to(share, (8, LANES))

    def pd_copies(src, dst, send, recv, name, here, count):
        return [pltpu.make_async_remote_copy(
            src_ref=src, dst_ref=dst.at[here], send_sem=send.at[d], recv_sem=recv.at[here],
            device_id={name: lax.rem(here + d, count)}, device_id_type=MESH)
            for d in range(1, count)]

    def pd_total(first, dst, recv, here, count):
        total = first[...]
        for d in range(1, count):
            other = lax.rem(here + d, count)
            arrived(dst.at[other], recv.at[other])
            total = total + dst[other]
        return total

    pdz = pd_copies(pd_z.at[n_rows], pd_z, pdz_send, pdz_recv, "rows", z, n_rows)
    pds = pd_copies(pd_own_s, pd_s, pds_send, pds_recv, "sub", s, n_sub)
    pdc = pd_copies(pd_own_c, pd_c, pdc_send, pdc_recv, "cols", x, n_cols)
    for c in pdz:
        c.start()

    load_prev.wait()
    prev_t[...] = jnp.transpose(prev[...].astype(jnp.float32))

    inner = (z > 0) & (z < n_rows - 1)
    tilt = jnp.where(inner, hop_lead * (2 * z - (n_rows - 1)), 0)
    wait_l = jnp.clip(tilt, 0, z_chunks)
    wait_r = jnp.clip(-tilt, 0, z_chunks)
    lag = jnp.maximum(wait_l, wait_r)
    most_lag = min(z_chunks, hop_lead * max(n_rows - 3, 0))

    def sub_copy(m, d):
        return pltpu.make_async_remote_copy(
            src_ref=sub_out.at[m, d], dst_ref=sub_in.at[m, s], send_sem=sub_send.at[m, d],
            recv_sem=sub_recv.at[m, s], device_id={"sub": lax.rem(s + d, n_sub)},
            device_id_type=MESH)

    def col_copy(m, d):
        return pltpu.make_async_remote_copy(
            src_ref=col_out.at[m, d], dst_ref=col_in.at[m, x], send_sem=col_send.at[m, d],
            recv_sem=col_recv.at[m, x], device_id={"cols": lax.rem(x + d, n_cols)},
            device_id_type=MESH)

    def block_dot(pivot_rows_t, col, sub):
        at = pl.multiple_of((col * n_sub + sub) * rows_here, LANES)
        return jnp.dot(
            pivot_rows_t, vec[:, pl.ds(at, rows_here)], preferred_element_type=jnp.float32)

    def multiply(m):
        rows = pl.ds(m * per_m, per_m)

        @pl.when(z < n_rows - 1)
        def _():
            pivot_t[rows] = fwd_r[rows] + from_r[rows]

        @pl.when(z == n_rows - 1)
        def _():
            pivot_t[rows] = fwd_r[rows]

        pt = pivot_t[rows].reshape(m_rows, width)
        for d in range(1, n_sub):
            for c in range(n_cols):
                sub_out[m, d, c] = block_dot(
                    pt, lax.rem(x + c, n_cols), lax.rem(s + d, n_sub))
            sub_copy(m, d).start()
        for c in range(1, n_cols):
            col_out[m, c] = block_dot(pt, lax.rem(x + c, n_cols), s)
        mine[m] = block_dot(pt, x, s)

    def reduce_chip(m):
        for d in range(1, n_sub):
            other = lax.rem(s + d, n_sub)
            arrived(sub_in.at[m, other], sub_recv.at[m, other])
        for c in range(1, n_cols):
            total = col_out[m, c]
            for d in range(1, n_sub):
                total = total + sub_in[m, lax.rem(s + d, n_sub), c]
            col_out[m, c] = total
            col_copy(m, c).start()
        total = mine[m]
        for d in range(1, n_sub):
            total = total + sub_in[m, lax.rem(s + d, n_sub), 0]
        mine[m] = total

    steps = most_lag + z_chunks + 1

    def step(t, carry):
        q_l, q_r, q_m = t - wait_l, t - wait_r, t - lag

        @pl.when((z > 0) & (q_l >= 0) & (q_l < z_chunks))
        def _():
            z_copy(fwd_r, from_l, zr_send, l_recv, q_l, 1).wait_recv()
            fwd_r[q_l] = from_l[q_l] + own[q_l]

            @pl.when(z < n_rows - 1)
            def _():
                z_copy(fwd_r, from_l, zr_send, l_recv, q_l, 1).start()

        @pl.when((z < n_rows - 1) & (q_r >= 0) & (q_r < z_chunks))
        def _():
            z_copy(fwd_l, from_r, zl_send, r_recv, q_r, -1).wait_recv()

            @pl.when(z > 0)
            def _():
                fwd_l[q_r] = from_r[q_r] + own[q_r]
                z_copy(fwd_l, from_r, zl_send, r_recv, q_r, -1).start()

        @pl.when(q_m == z_chunks - 1)
        def _():
            for d in (1, n_rows - 1):
                @pl.when(near(d))
                def _():
                    ket_copy(d).start()

        @pl.when((q_m >= per_m) & (q_m <= z_chunks) & (lax.rem(q_m, per_m) == 0))
        def _():
            reduce_chip(q_m // per_m - 1)

        @pl.when((q_m >= 0) & (q_m < z_chunks) & (lax.rem(q_m, per_m) == per_m - 1))
        def _():
            multiply(q_m // per_m)

        @pl.when(t == z_chunks // 2)
        def _():
            pd_own_s[...] = pd_total(pd_z.at[n_rows], pd_z, pdz_recv, z, n_rows)
            for c in pds:
                c.start()

        @pl.when(t == z_chunks - 1)
        def _():
            pd_own_c[...] = pd_total(pd_own_s, pd_s, pds_recv, s, n_sub)
            for c in pdc:
                c.start()

        return carry

    lax.fori_loop(0, steps, step, 0)

    pivot_diag = pd_total(pd_own_c, pd_c, pdc_recv, x, n_cols)
    inverse = 1.0 / jnp.sqrt(column_of(pivot_diag[0:1, :]))
    total_sq = jnp.zeros((1, rows_here), jnp.float32)
    per_t = max(LANES // m_rows, 1)
    for m in range(m_chunks):
        if m == m_chunks - 1:
            for d in range(1, n_rows):
                other = lax.rem(z + d, n_rows)
                arrived(landed.at[other], ket_recv.at[other])
            for place in range(per_device):
                block = device * per_device + place
                source = jnp.int32(0)
                for band in range(n_rows):
                    owner = band * column_size + column
                    for slot in range(slot_count):
                        fits = (slot < counts_ref[owner]) & (targets_ref[owner, slot] == block)
                        source = jnp.where(fits, jnp.int32(band), source)
                next_ref[place * block_rows:(place + 1) * block_rows, :] = landed[source]
        total = mine[m]
        for c in range(1, n_cols):
            other = lax.rem(x + c, n_cols)
            arrived(col_in.at[m, other], col_recv.at[m, other])
            total = total + col_in[m, other]
        rows = slice(m * m_rows, (m + 1) * m_rows)
        for h in range(rows_here // LANES):
            cut = slice(h * LANES, (h + 1) * LANES)
            scaled_t[rows, cut] = (prev_t[rows, cut] - total[:, cut]) * inverse[rows, :]
        scaled = scaled_t[rows, :]
        total_sq = total_sq + jnp.sum(scaled * scaled, axis=0, keepdims=True)
        if (m + 1) % per_t == 0:
            done = slice((m + 1 - per_t) * m_rows, (m + 1) * m_rows)
            new_ref[:, done] = jnp.transpose(scaled_t[done, :]).astype(jnp.bfloat16)
    diag_out_ref[...] = diag_ref[...] - total_sq

    for c in pdz + pds + pdc:
        c.wait_send()
    for d in range(1, n_rows):
        ket_copy(d).wait_send()

    @pl.when(z < n_rows - 1)
    def _():
        for q in range(z_chunks):
            z_copy(own, from_l, zr_send, l_recv, q, 1).wait_send()

    @pl.when(z > 0)
    def _():
        for q in range(z_chunks):
            z_copy(own, from_r, zl_send, r_recv, q, -1).wait_send()

    for m in range(m_chunks):
        for d in range(1, n_sub):
            sub_copy(m, d).wait_send()
        for c in range(1, n_cols):
            col_copy(m, c).wait_send()


def body(mesh_sizes, vectors, previous, pivots, diagonal, ket_blocks, tags, targets, counts, norms):
    n_rows, n_cols, n_sub = mesh_sizes
    width, band_rows = vectors.shape
    rows_here, batch = previous.shape
    slot_count, block_rows, _ = ket_blocks.shape
    z_chunks, m_chunks, hop_lead = 8, 4, 3
    z_rows, m_rows = batch // z_chunks, batch // m_chunks
    f32, bf16, dma = jnp.float32, jnp.bfloat16, pltpu.SemaphoreType.DMA
    line = pltpu.VMEM((z_chunks, z_rows, width), bf16)
    small = pltpu.VMEM((8, batch), f32)
    scratch = [
        pltpu.VMEM(vectors.shape, bf16), pltpu.VMEM(previous.shape, bf16),
        pltpu.VMEM(ket_blocks.shape, bf16), pltpu.VMEM((batch, band_rows), bf16),
        line, line, line, line, line, line,
        pltpu.VMEM((batch, rows_here), f32),
        pltpu.VMEM((m_chunks, n_sub, n_cols, m_rows, rows_here), f32),
        pltpu.VMEM((m_chunks, n_sub, n_cols, m_rows, rows_here), f32),
        pltpu.VMEM((m_chunks, m_rows, rows_here), f32),
        pltpu.VMEM((m_chunks, n_cols, m_rows, rows_here), f32),
        pltpu.VMEM((m_chunks, n_cols, m_rows, rows_here), f32),
        pltpu.VMEM((batch, rows_here), f32),
        pltpu.VMEM((n_rows, block_rows, batch), bf16),
        pltpu.VMEM((n_rows, block_rows, batch), bf16),
        pltpu.VMEM((n_rows + 1, 8, batch), f32), pltpu.VMEM((n_sub, 8, batch), f32),
        pltpu.VMEM((n_cols, 8, batch), f32), small, small,
        dma((3,)), dma((z_chunks,)), dma((z_chunks,)), dma((z_chunks,)), dma((z_chunks,)),
        dma((m_chunks, n_sub)), dma((m_chunks, n_sub)),
        dma((m_chunks, n_cols)), dma((m_chunks, n_cols)),
        dma((n_rows,)), dma((n_rows,)), dma((n_rows,)), dma((n_rows,)),
        dma((n_sub,)), dma((n_sub,)), dma((n_cols,)), dma((n_cols,)),
    ]
    hbm = pl.BlockSpec(memory_space=pl.ANY)
    vmem = pl.BlockSpec(memory_space=pltpu.VMEM)
    smem = pl.BlockSpec(memory_space=pltpu.SMEM)
    new_vectors, diag_out, next_columns = pl.pallas_call(
        functools.partial(kernel, (n_rows, n_cols, n_sub, hop_lead)),
        out_shape=(
            jax.ShapeDtypeStruct((rows_here, batch), bf16),
            jax.ShapeDtypeStruct((1, rows_here), f32),
            jax.ShapeDtypeStruct((rows_here, batch), bf16),
        ),
        in_specs=[hbm, hbm, vmem, vmem, hbm, vmem, smem, smem, smem],
        out_specs=(vmem, vmem, vmem),
        scratch_shapes=scratch,
        compiler_params=pltpu.CompilerParams(
            collective_id=0, has_side_effects=True, vmem_limit_bytes=48 * 1024 * 1024),
    )(
        vectors, previous, pivots.reshape(1, batch), diagonal.reshape(1, rows_here),
        ket_blocks, tags, targets, counts, norms,
    )
    return new_vectors, diag_out.reshape(rows_here), next_columns


def solution(mesh):
    sizes = tuple(mesh.shape[name] for name in ("rows", "cols", "sub"))
    return jax.shard_map(
        functools.partial(body, sizes),
        mesh=mesh,
        in_specs=(
            P(("cols", "sub"), ("groups", "rows")),
            P(("groups", "rows", "cols", "sub"), None),
            P("groups"),
            P(("groups", "rows", "cols", "sub")),
            P(("groups", "rows", "cols", "sub"), None, None),
            P(("groups", "rows", "cols", "sub"), None),
            P("groups", None),
            P("groups"),
            P(),
        ),
        out_specs=(
            P(("groups", "rows", "cols", "sub"), None),
            P(("groups", "rows", "cols", "sub")),
            P(("groups", "rows", "cols", "sub"), None),
        ),
        check_vma=False,
    )
```

```python
import functools

import jax
import jax.numpy as jnp
from jax import lax
from jax.experimental import pallas as pl
from jax.experimental.pallas import tpu as pltpu
from jax.sharding import PartitionSpec as P

MESH = pl.DeviceIdType.MESH
LANES = 128


def column_of(row):
    return jnp.transpose(jnp.broadcast_to(row, (LANES, row.shape[1])))


def kernel(
    sizes,
    vec_hbm, prev_hbm, piv_ref, diag_ref, ket_hbm, tags_ref, targets_ref, counts_ref, norms_ref,
    new_ref, diag_out_ref, next_ref,
    vec, prev, ket, hot, own, fwd_r, fwd_l, from_l, from_r,
    pivot_t, prev_t, sub_out, sub_in, mine, col_out, col_in, scaled_t,
    stage, landed, pd_z, pd_s, pd_c, pd_own_s, pd_own_c,
    load_sem, zr_send, zl_send, l_recv, r_recv, sub_send, sub_recv, col_send, col_recv,
    ket_send, ket_recv, pdz_send, pdz_recv, pds_send, pds_recv, pdc_send, pdc_recv,
):
    n_rows, n_cols, n_sub, hop_lead = sizes
    z, x, s = lax.axis_index("rows"), lax.axis_index("cols"), lax.axis_index("sub")
    column_size = n_cols * n_sub
    column = x * n_sub + s
    device = z * column_size + column
    slot_count, block_rows, batch = ket_hbm.shape
    rows_here = prev_hbm.shape[0]
    per_device = rows_here // block_rows
    width, band_rows = vec_hbm.shape
    z_chunks, z_rows = own.shape[0], own.shape[1]
    m_chunks, m_rows = mine.shape[0], mine.shape[1]
    per_m = m_rows // z_rows

    load_ket = pltpu.make_async_copy(ket_hbm, ket, load_sem.at[0])
    load_vec = pltpu.make_async_copy(vec_hbm, vec, load_sem.at[1])
    load_prev = pltpu.make_async_copy(prev_hbm, prev, load_sem.at[2])
    load_ket.start()
    load_vec.start()
    load_prev.start()

    barrier = pltpu.get_barrier_semaphore()
    for name, here, count in (("rows", z, n_rows), ("cols", x, n_cols), ("sub", s, n_sub)):
        for d in range(1, count):
            pl.semaphore_signal(
                barrier, inc=1, device_id={name: lax.rem(here + d, count)}, device_id_type=MESH
            )

    piv_col = column_of(piv_ref[...].astype(jnp.float32)).astype(jnp.int32) - z * band_rows
    lane = lax.broadcasted_iota(jnp.int32, (batch, LANES), 1)
    for t in range(band_rows // LANES):
        hot[:, t * LANES:(t + 1) * LANES] = (piv_col == lane + t * LANES).astype(
            jnp.float32).astype(jnp.bfloat16)

    tags = tags_ref[...]
    factor = jnp.zeros(tags.shape, jnp.float32)
    for kind in range(norms_ref.shape[0]):
        factor = jnp.where(tags == kind, norms_ref[kind], factor)
    load_ket.wait()
    for slot in range(slot_count):
        scale = column_of(factor[slot:slot + 1, :])
        for h in range(batch // LANES):
            part = (slot, slice(None), slice(h * LANES, (h + 1) * LANES))
            ket[part] = (ket[part].astype(jnp.float32) * scale).astype(jnp.bfloat16)
    used = counts_ref[device]

    def stage_for(band):
        low = (band * column_size + column) * per_device
        chosen = jnp.int32(0)
        for slot in range(slot_count):
            target = targets_ref[slot, device]
            fits = (slot < used) & (target >= low) & (target < low + per_device)
            chosen = jnp.where(fits, jnp.int32(slot), chosen)
        return ket[chosen]

    landed[z] = stage_for(z)
    for d in range(1, n_rows):
        stage[d] = stage_for(lax.rem(z + d, n_rows))

    def ket_copy(d):
        return pltpu.make_async_remote_copy(
            src_ref=stage.at[d], dst_ref=landed.at[z], send_sem=ket_send.at[d],
            recv_sem=ket_recv.at[z], device_id={"rows": lax.rem(z + d, n_rows)},
            device_id_type=MESH)

    pl.semaphore_wait(barrier, n_rows + n_cols + n_sub - 3)

    def near(d):
        right = z < n_rows - 1 if d == 1 else False
        left = z > 0 if d == n_rows - 1 else False
        return jnp.logical_or(right, left)

    for d in range(1, n_rows):
        @pl.when(jnp.logical_not(near(d)))
        def _():
            ket_copy(d).start()

    def z_copy(src, dst, send, recv, q, dz):
        return pltpu.make_async_remote_copy(
            src_ref=src.at[q], dst_ref=dst.at[q], send_sem=send.at[q], recv_sem=recv.at[q],
            device_id={"rows": lax.rem(z + dz + n_rows, n_rows)}, device_id_type=MESH)

    def arrived(dst, sem):
        pltpu.make_async_remote_copy(
            src_ref=dst, dst_ref=dst, send_sem=sem, recv_sem=sem,
            device_id={"sub": lax.rem(s + 1, n_sub)}, device_id_type=MESH).wait_recv()

    load_vec.wait()
    piece = min(LANES, batch)
    in_piece = piece // z_rows
    for p in range(batch // piece):
        got = lax.dot_general(
            hot[p * piece:(p + 1) * piece, :], vec[...], (((1,), (1,)), ((), ())),
            preferred_element_type=jnp.float32).astype(jnp.bfloat16)
        got = got.reshape(in_piece, z_rows, width)
        own[p * in_piece:(p + 1) * in_piece] = got

        @pl.when(z == 0)
        def _():
            fwd_r[p * in_piece:(p + 1) * in_piece] = got
            for q in range(p * in_piece, (p + 1) * in_piece):
                z_copy(own, from_l, zr_send, l_recv, q, 1).start()

        @pl.when(z == n_rows - 1)
        def _():
            for q in range(p * in_piece, (p + 1) * in_piece):
                z_copy(own, from_r, zl_send, r_recv, q, -1).start()

    diag_col = column_of(diag_ref[...])
    row = lax.broadcasted_iota(jnp.int32, (rows_here, LANES), 0) + device * rows_here
    for h in range(batch // LANES):
        cut = slice(h * LANES, (h + 1) * LANES)
        share = jnp.sum(jnp.where(piv_ref[:, cut] == row, diag_col, 0.0), axis=0, keepdims=True)
        pd_z[n_rows, :, cut] = jnp.broadcast_to(share, (8, LANES))

    def pd_copies(src, dst, send, recv, name, here, count):
        return [pltpu.make_async_remote_copy(
            src_ref=src, dst_ref=dst.at[here], send_sem=send.at[d], recv_sem=recv.at[here],
            device_id={name: lax.rem(here + d, count)}, device_id_type=MESH)
            for d in range(1, count)]

    def pd_total(first, dst, recv, here, count):
        total = first[...]
        for d in range(1, count):
            other = lax.rem(here + d, count)
            arrived(dst.at[other], recv.at[other])
            total = total + dst[other]
        return total

    pdz = pd_copies(pd_z.at[n_rows], pd_z, pdz_send, pdz_recv, "rows", z, n_rows)
    pds = pd_copies(pd_own_s, pd_s, pds_send, pds_recv, "sub", s, n_sub)
    pdc = pd_copies(pd_own_c, pd_c, pdc_send, pdc_recv, "cols", x, n_cols)
    for c in pdz:
        c.start()

    load_prev.wait()
    prev_t[...] = jnp.transpose(prev[...].astype(jnp.float32))

    inner = (z > 0) & (z < n_rows - 1)
    tilt = jnp.where(inner, hop_lead * (2 * z - (n_rows - 1)), 0)
    wait_l = jnp.clip(tilt, 0, z_chunks)
    wait_r = jnp.clip(-tilt, 0, z_chunks)
    lag = jnp.maximum(wait_l, wait_r)
    most_lag = min(z_chunks, hop_lead * max(n_rows - 3, 0))

    def sub_copy(m, d):
        return pltpu.make_async_remote_copy(
            src_ref=sub_out.at[m, d], dst_ref=sub_in.at[m, s], send_sem=sub_send.at[m, d],
            recv_sem=sub_recv.at[m, s], device_id={"sub": lax.rem(s + d, n_sub)},
            device_id_type=MESH)

    def col_copy(m, d):
        return pltpu.make_async_remote_copy(
            src_ref=col_out.at[m, d], dst_ref=col_in.at[m, x], send_sem=col_send.at[m, d],
            recv_sem=col_recv.at[m, x], device_id={"cols": lax.rem(x + d, n_cols)},
            device_id_type=MESH)

    def block_dot(pivot_rows_t, col, sub):
        at = pl.multiple_of((col * n_sub + sub) * rows_here, LANES)
        return jnp.dot(
            pivot_rows_t, vec[:, pl.ds(at, rows_here)], preferred_element_type=jnp.float32)

    def multiply(m):
        rows = pl.ds(m * per_m, per_m)

        @pl.when(z < n_rows - 1)
        def _():
            pivot_t[rows] = fwd_r[rows] + from_r[rows]

        @pl.when(z == n_rows - 1)
        def _():
            pivot_t[rows] = fwd_r[rows]

        pt = pivot_t[rows].reshape(m_rows, width)
        for d in range(1, n_sub):
            for c in range(n_cols):
                sub_out[m, d, c] = block_dot(
                    pt, lax.rem(x + c, n_cols), lax.rem(s + d, n_sub))
            sub_copy(m, d).start()
        for c in range(1, n_cols):
            col_out[m, c] = block_dot(pt, lax.rem(x + c, n_cols), s)
        mine[m] = block_dot(pt, x, s)

    def reduce_chip(m):
        for d in range(1, n_sub):
            other = lax.rem(s + d, n_sub)
            arrived(sub_in.at[m, other], sub_recv.at[m, other])
        for c in range(1, n_cols):
            total = col_out[m, c]
            for d in range(1, n_sub):
                total = total + sub_in[m, lax.rem(s + d, n_sub), c]
            col_out[m, c] = total
            col_copy(m, c).start()
        total = mine[m]
        for d in range(1, n_sub):
            total = total + sub_in[m, lax.rem(s + d, n_sub), 0]
        mine[m] = total

    steps = most_lag + z_chunks + 1

    def step(t, carry):
        q_l, q_r, q_m = t - wait_l, t - wait_r, t - lag

        @pl.when((z > 0) & (q_l >= 0) & (q_l < z_chunks))
        def _():
            z_copy(fwd_r, from_l, zr_send, l_recv, q_l, 1).wait_recv()
            fwd_r[q_l] = from_l[q_l] + own[q_l]

            @pl.when(z < n_rows - 1)
            def _():
                z_copy(fwd_r, from_l, zr_send, l_recv, q_l, 1).start()

        @pl.when((z < n_rows - 1) & (q_r >= 0) & (q_r < z_chunks))
        def _():
            z_copy(fwd_l, from_r, zl_send, r_recv, q_r, -1).wait_recv()

            @pl.when(z > 0)
            def _():
                fwd_l[q_r] = from_r[q_r] + own[q_r]
                z_copy(fwd_l, from_r, zl_send, r_recv, q_r, -1).start()

        @pl.when(q_m == z_chunks - 1)
        def _():
            for d in (1, n_rows - 1):
                @pl.when(near(d))
                def _():
                    ket_copy(d).start()

        @pl.when((q_m >= per_m) & (q_m <= z_chunks) & (lax.rem(q_m, per_m) == 0))
        def _():
            reduce_chip(q_m // per_m - 1)

        @pl.when((q_m >= 0) & (q_m < z_chunks) & (lax.rem(q_m, per_m) == per_m - 1))
        def _():
            multiply(q_m // per_m)

        @pl.when(t == z_chunks // 2)
        def _():
            pd_own_s[...] = pd_total(pd_z.at[n_rows], pd_z, pdz_recv, z, n_rows)
            for c in pds:
                c.start()

        @pl.when(t == z_chunks - 1)
        def _():
            pd_own_c[...] = pd_total(pd_own_s, pd_s, pds_recv, s, n_sub)
            for c in pdc:
                c.start()

        return carry

    lax.fori_loop(0, steps, step, 0)

    pivot_diag = pd_total(pd_own_c, pd_c, pdc_recv, x, n_cols)
    inverse = 1.0 / jnp.sqrt(column_of(pivot_diag[0:1, :]))
    total_sq = jnp.zeros((1, rows_here), jnp.float32)
    per_t = max(LANES // m_rows, 1)
    for m in range(m_chunks):
        if m == m_chunks - 1:
            for d in range(1, n_rows):
                other = lax.rem(z + d, n_rows)
                arrived(landed.at[other], ket_recv.at[other])
            for place in range(per_device):
                block = device * per_device + place
                source = jnp.int32(0)
                for band in range(n_rows):
                    owner = band * column_size + column
                    for slot in range(slot_count):
                        fits = (slot < counts_ref[owner]) & (targets_ref[slot, owner] == block)
                        source = jnp.where(fits, jnp.int32(band), source)
                next_ref[place * block_rows:(place + 1) * block_rows, :] = landed[source]
        total = mine[m]
        for c in range(1, n_cols):
            other = lax.rem(x + c, n_cols)
            arrived(col_in.at[m, other], col_recv.at[m, other])
            total = total + col_in[m, other]
        rows = slice(m * m_rows, (m + 1) * m_rows)
        for h in range(rows_here // LANES):
            cut = slice(h * LANES, (h + 1) * LANES)
            scaled_t[rows, cut] = (prev_t[rows, cut] - total[:, cut]) * inverse[rows, :]
        scaled = scaled_t[rows, :]
        total_sq = total_sq + jnp.sum(scaled * scaled, axis=0, keepdims=True)
        if (m + 1) % per_t == 0:
            done = slice((m + 1 - per_t) * m_rows, (m + 1) * m_rows)
            new_ref[:, done] = jnp.transpose(scaled_t[done, :]).astype(jnp.bfloat16)
    diag_out_ref[...] = diag_ref[...] - total_sq

    for c in pdz + pds + pdc:
        c.wait_send()
    for d in range(1, n_rows):
        ket_copy(d).wait_send()

    @pl.when(z < n_rows - 1)
    def _():
        for q in range(z_chunks):
            z_copy(own, from_l, zr_send, l_recv, q, 1).wait_send()

    @pl.when(z > 0)
    def _():
        for q in range(z_chunks):
            z_copy(own, from_r, zl_send, r_recv, q, -1).wait_send()

    for m in range(m_chunks):
        for d in range(1, n_sub):
            sub_copy(m, d).wait_send()
        for c in range(1, n_cols):
            col_copy(m, c).wait_send()


def body(mesh_sizes, vectors, previous, pivots, diagonal, ket_blocks, tags, targets, counts, norms):
    n_rows, n_cols, n_sub = mesh_sizes
    width, band_rows = vectors.shape
    rows_here, batch = previous.shape
    slot_count, block_rows, _ = ket_blocks.shape
    z_chunks, m_chunks, hop_lead = 8, 4, 3
    z_rows, m_rows = batch // z_chunks, batch // m_chunks
    f32, bf16, dma = jnp.float32, jnp.bfloat16, pltpu.SemaphoreType.DMA
    line = pltpu.VMEM((z_chunks, z_rows, width), bf16)
    small = pltpu.VMEM((8, batch), f32)
    scratch = [
        pltpu.VMEM(vectors.shape, bf16), pltpu.VMEM(previous.shape, bf16),
        pltpu.VMEM(ket_blocks.shape, bf16), pltpu.VMEM((batch, band_rows), bf16),
        line, line, line, line, line, line,
        pltpu.VMEM((batch, rows_here), f32),
        pltpu.VMEM((m_chunks, n_sub, n_cols, m_rows, rows_here), f32),
        pltpu.VMEM((m_chunks, n_sub, n_cols, m_rows, rows_here), f32),
        pltpu.VMEM((m_chunks, m_rows, rows_here), f32),
        pltpu.VMEM((m_chunks, n_cols, m_rows, rows_here), f32),
        pltpu.VMEM((m_chunks, n_cols, m_rows, rows_here), f32),
        pltpu.VMEM((batch, rows_here), f32),
        pltpu.VMEM((n_rows, block_rows, batch), bf16),
        pltpu.VMEM((n_rows, block_rows, batch), bf16),
        pltpu.VMEM((n_rows + 1, 8, batch), f32), pltpu.VMEM((n_sub, 8, batch), f32),
        pltpu.VMEM((n_cols, 8, batch), f32), small, small,
        dma((3,)), dma((z_chunks,)), dma((z_chunks,)), dma((z_chunks,)), dma((z_chunks,)),
        dma((m_chunks, n_sub)), dma((m_chunks, n_sub)),
        dma((m_chunks, n_cols)), dma((m_chunks, n_cols)),
        dma((n_rows,)), dma((n_rows,)), dma((n_rows,)), dma((n_rows,)),
        dma((n_sub,)), dma((n_sub,)), dma((n_cols,)), dma((n_cols,)),
    ]
    hbm = pl.BlockSpec(memory_space=pl.ANY)
    vmem = pl.BlockSpec(memory_space=pltpu.VMEM)
    smem = pl.BlockSpec(memory_space=pltpu.SMEM)
    new_vectors, diag_out, next_columns = pl.pallas_call(
        functools.partial(kernel, (n_rows, n_cols, n_sub, hop_lead)),
        out_shape=(
            jax.ShapeDtypeStruct((rows_here, batch), bf16),
            jax.ShapeDtypeStruct((1, rows_here), f32),
            jax.ShapeDtypeStruct((rows_here, batch), bf16),
        ),
        in_specs=[hbm, hbm, vmem, vmem, hbm, vmem, smem, smem, smem],
        out_specs=(vmem, vmem, vmem),
        scratch_shapes=scratch,
        compiler_params=pltpu.CompilerParams(
            collective_id=0, has_side_effects=True, vmem_limit_bytes=67043328),
    )(
        vectors, previous, pivots.reshape(1, batch), diagonal.reshape(1, rows_here),
        ket_blocks, tags, targets.T, counts, norms,
    )
    return new_vectors, diag_out.reshape(rows_here), next_columns


def solution(mesh):
    sizes = tuple(mesh.shape[name] for name in ("rows", "cols", "sub"))
    return jax.shard_map(
        functools.partial(body, sizes),
        mesh=mesh,
        in_specs=(
            P(("cols", "sub"), ("groups", "rows")),
            P(("groups", "rows", "cols", "sub"), None),
            P("groups"),
            P(("groups", "rows", "cols", "sub")),
            P(("groups", "rows", "cols", "sub"), None, None),
            P(("groups", "rows", "cols", "sub"), None),
            P("groups", None),
            P("groups"),
            P(),
        ),
        out_specs=(
            P(("groups", "rows", "cols", "sub"), None),
            P(("groups", "rows", "cols", "sub")),
            P(("groups", "rows", "cols", "sub"), None),
        ),
        check_vma=False,
    )
```

```python
import functools

import jax
import jax.numpy as jnp
from jax import lax
from jax.experimental import pallas as pl
from jax.experimental.pallas import tpu as pltpu
from jax.sharding import PartitionSpec as P

MESH = pl.DeviceIdType.MESH
LANES = 128


def column_of(row):
    return jnp.transpose(jnp.broadcast_to(row, (LANES, row.shape[1])))


def kernel(
    sizes,
    vec_hbm, prev_hbm, piv_ref, diag_ref, ket_hbm, tags_ref, targets_ref, counts_ref, norms_ref,
    new_ref, diag_out_ref, next_ref,
    vec, prev, ket, hot, own, fwd_r, fwd_l, from_l, from_r,
    pivot_t, prev_t, sub_out, sub_in, mine, col_out, col_in, scaled_t,
    stage, landed, pd_z, pd_s, pd_c, pd_own_s, pd_own_c,
    load_sem, zr_send, zl_send, l_recv, r_recv, sub_send, sub_recv, col_send, col_recv,
    ket_send, ket_recv, pdz_send, pdz_recv, pds_send, pds_recv, pdc_send, pdc_recv,
):
    n_rows, n_cols, n_sub, hop_lead = sizes
    z, x, s = lax.axis_index("rows"), lax.axis_index("cols"), lax.axis_index("sub")
    column_size = n_cols * n_sub
    column = x * n_sub + s
    device = z * column_size + column
    slot_count, block_rows, batch = ket_hbm.shape
    rows_here = prev_hbm.shape[0]
    per_device = rows_here // block_rows
    width, band_rows = vec_hbm.shape
    z_chunks, z_rows = own.shape[0], own.shape[1]
    m_chunks, m_rows = mine.shape[0], mine.shape[1]
    per_m = m_rows // z_rows

    load_ket = pltpu.make_async_copy(ket_hbm, ket, load_sem.at[0])
    load_vec = pltpu.make_async_copy(vec_hbm, vec, load_sem.at[1])
    load_prev = pltpu.make_async_copy(prev_hbm, prev, load_sem.at[2])
    load_ket.start()
    load_vec.start()
    load_prev.start()

    barrier = pltpu.get_barrier_semaphore()
    for name, here, count in (("rows", z, n_rows), ("cols", x, n_cols), ("sub", s, n_sub)):
        for d in range(1, count):
            pl.semaphore_signal(
                barrier, inc=1, device_id={name: lax.rem(here + d, count)}, device_id_type=MESH
            )

    piv_col = column_of(piv_ref[...].astype(jnp.float32)).astype(jnp.int32) - z * band_rows
    lane = lax.broadcasted_iota(jnp.int32, (batch, LANES), 1)
    for t in range(band_rows // LANES):
        hot[:, t * LANES:(t + 1) * LANES] = (piv_col == lane + t * LANES).astype(
            jnp.float32).astype(jnp.bfloat16)

    diag_col = column_of(diag_ref[...])
    row = lax.broadcasted_iota(jnp.int32, (rows_here, LANES), 0) + device * rows_here
    for h in range(batch // LANES):
        cut = slice(h * LANES, (h + 1) * LANES)
        share = jnp.sum(jnp.where(piv_ref[:, cut] == row, diag_col, 0.0), axis=0, keepdims=True)
        pd_z[n_rows, :, cut] = jnp.broadcast_to(share, (8, LANES))

    tags = tags_ref[...]
    factor = jnp.zeros(tags.shape, jnp.float32)
    for kind in range(norms_ref.shape[0]):
        factor = jnp.where(tags == kind, norms_ref[kind], factor)
    load_ket.wait()
    for slot in range(slot_count):
        scale = column_of(factor[slot:slot + 1, :])
        for h in range(batch // LANES):
            part = (slot, slice(None), slice(h * LANES, (h + 1) * LANES))
            ket[part] = (ket[part].astype(jnp.float32) * scale).astype(jnp.bfloat16)
    used = counts_ref[device]

    def stage_for(band):
        low = (band * column_size + column) * per_device
        chosen = jnp.int32(0)
        for slot in range(slot_count):
            target = targets_ref[slot, device]
            fits = (slot < used) & (target >= low) & (target < low + per_device)
            chosen = jnp.where(fits, jnp.int32(slot), chosen)
        return ket[chosen]

    landed[z] = stage_for(z)
    for d in range(1, n_rows):
        stage[d] = stage_for(lax.rem(z + d, n_rows))

    def ket_copy(d):
        return pltpu.make_async_remote_copy(
            src_ref=stage.at[d], dst_ref=landed.at[z], send_sem=ket_send.at[d],
            recv_sem=ket_recv.at[z], device_id={"rows": lax.rem(z + d, n_rows)},
            device_id_type=MESH)

    pl.semaphore_wait(barrier, n_rows + n_cols + n_sub - 3)

    def pd_copies(src, dst, send, recv, name, here, count):
        return [pltpu.make_async_remote_copy(
            src_ref=src, dst_ref=dst.at[here], send_sem=send.at[d], recv_sem=recv.at[here],
            device_id={name: lax.rem(here + d, count)}, device_id_type=MESH)
            for d in range(1, count)]

    pdz = pd_copies(pd_z.at[n_rows], pd_z, pdz_send, pdz_recv, "rows", z, n_rows)
    pds = pd_copies(pd_own_s, pd_s, pds_send, pds_recv, "sub", s, n_sub)
    pdc = pd_copies(pd_own_c, pd_c, pdc_send, pdc_recv, "cols", x, n_cols)
    for c in pdz:
        c.start()

    inner = (z > 0) & (z < n_rows - 1)

    @pl.when(inner)
    def _():
        for d in range(1, n_rows):
            ket_copy(d).start()

    def z_copy(src, dst, send, recv, q, dz):
        return pltpu.make_async_remote_copy(
            src_ref=src.at[q], dst_ref=dst.at[q], send_sem=send.at[q], recv_sem=recv.at[q],
            device_id={"rows": lax.rem(z + dz + n_rows, n_rows)}, device_id_type=MESH)

    def arrived(dst, sem):
        pltpu.make_async_remote_copy(
            src_ref=dst, dst_ref=dst, send_sem=sem, recv_sem=sem,
            device_id={"sub": lax.rem(s + 1, n_sub)}, device_id_type=MESH).wait_recv()

    load_vec.wait()
    piece = min(LANES, batch)
    in_piece = piece // z_rows
    for p in range(batch // piece):
        got = lax.dot_general(
            hot[p * piece:(p + 1) * piece, :], vec[...], (((1,), (1,)), ((), ())),
            preferred_element_type=jnp.float32).astype(jnp.bfloat16)
        got = got.reshape(in_piece, z_rows, width)
        own[p * in_piece:(p + 1) * in_piece] = got

        @pl.when(z == 0)
        def _():
            fwd_r[p * in_piece:(p + 1) * in_piece] = got
            for q in range(p * in_piece, (p + 1) * in_piece):
                z_copy(own, from_l, zr_send, l_recv, q, 1).start()

        @pl.when(z == n_rows - 1)
        def _():
            for q in range(p * in_piece, (p + 1) * in_piece):
                z_copy(own, from_r, zl_send, r_recv, q, -1).start()

    def pd_total(first, dst, recv, here, count):
        total = first[...]
        for d in range(1, count):
            other = lax.rem(here + d, count)
            arrived(dst.at[other], recv.at[other])
            total = total + dst[other]
        return total

    load_prev.wait()
    prev_t[...] = jnp.transpose(prev[...].astype(jnp.float32))

    tilt = jnp.where(inner, hop_lead * (2 * z - (n_rows - 1)), 0)
    wait_l = jnp.clip(tilt, 0, z_chunks)
    wait_r = jnp.clip(-tilt, 0, z_chunks)
    lag = jnp.maximum(wait_l, wait_r)
    most_lag = min(z_chunks, hop_lead * max(n_rows - 3, 0))

    def sub_copy(m, d):
        return pltpu.make_async_remote_copy(
            src_ref=sub_out.at[m, d], dst_ref=sub_in.at[m, s], send_sem=sub_send.at[m, d],
            recv_sem=sub_recv.at[m, s], device_id={"sub": lax.rem(s + d, n_sub)},
            device_id_type=MESH)

    def col_copy(m, d):
        return pltpu.make_async_remote_copy(
            src_ref=col_out.at[m, d], dst_ref=col_in.at[m, x], send_sem=col_send.at[m, d],
            recv_sem=col_recv.at[m, x], device_id={"cols": lax.rem(x + d, n_cols)},
            device_id_type=MESH)

    def block_dot(pivot_rows_t, col, sub):
        at = pl.multiple_of((col * n_sub + sub) * rows_here, LANES)
        return jnp.dot(
            pivot_rows_t, vec[:, pl.ds(at, rows_here)], preferred_element_type=jnp.float32)

    def multiply(m):
        rows = pl.ds(m * per_m, per_m)

        @pl.when(z < n_rows - 1)
        def _():
            pivot_t[rows] = fwd_r[rows] + from_r[rows]

        @pl.when(z == n_rows - 1)
        def _():
            pivot_t[rows] = fwd_r[rows]

        pt = pivot_t[rows].reshape(m_rows, width)
        for d in range(1, n_sub):
            for c in range(n_cols):
                sub_out[m, d, c] = block_dot(
                    pt, lax.rem(x + c, n_cols), lax.rem(s + d, n_sub))
            sub_copy(m, d).start()
        for c in range(1, n_cols):
            col_out[m, c] = block_dot(pt, lax.rem(x + c, n_cols), s)
        mine[m] = block_dot(pt, x, s)

    def reduce_chip(m):
        for d in range(1, n_sub):
            other = lax.rem(s + d, n_sub)
            arrived(sub_in.at[m, other], sub_recv.at[m, other])
        for c in range(1, n_cols):
            total = col_out[m, c]
            for d in range(1, n_sub):
                total = total + sub_in[m, lax.rem(s + d, n_sub), c]
            col_out[m, c] = total
            col_copy(m, c).start()
        total = mine[m]
        for d in range(1, n_sub):
            total = total + sub_in[m, lax.rem(s + d, n_sub), 0]
        mine[m] = total

    steps = most_lag + z_chunks + 1

    def step(t, carry):
        q_l, q_r, q_m = t - wait_l, t - wait_r, t - lag

        @pl.when((z > 0) & (q_l >= 0) & (q_l < z_chunks))
        def _():
            z_copy(fwd_r, from_l, zr_send, l_recv, q_l, 1).wait_recv()
            fwd_r[q_l] = from_l[q_l] + own[q_l]

            @pl.when(z < n_rows - 1)
            def _():
                z_copy(fwd_r, from_l, zr_send, l_recv, q_l, 1).start()

        @pl.when((z < n_rows - 1) & (q_r >= 0) & (q_r < z_chunks))
        def _():
            z_copy(fwd_l, from_r, zl_send, r_recv, q_r, -1).wait_recv()

            @pl.when(z > 0)
            def _():
                fwd_l[q_r] = from_r[q_r] + own[q_r]
                z_copy(fwd_l, from_r, zl_send, r_recv, q_r, -1).start()

        @pl.when(jnp.logical_not(inner) & (q_m == z_chunks - 2))
        def _():
            for d in range(1, n_rows):
                ket_copy(d).start()

        @pl.when((q_m >= per_m) & (q_m <= z_chunks) & (lax.rem(q_m, per_m) == 0))
        def _():
            reduce_chip(q_m // per_m - 1)

        @pl.when((q_m >= 0) & (q_m < z_chunks) & (lax.rem(q_m, per_m) == per_m - 1))
        def _():
            multiply(q_m // per_m)

        @pl.when(t == z_chunks // 2)
        def _():
            pd_own_s[...] = pd_total(pd_z.at[n_rows], pd_z, pdz_recv, z, n_rows)
            for c in pds:
                c.start()

        @pl.when(t == z_chunks - 1)
        def _():
            pd_own_c[...] = pd_total(pd_own_s, pd_s, pds_recv, s, n_sub)
            for c in pdc:
                c.start()

        return carry

    lax.fori_loop(0, steps, step, 0)

    pivot_diag = pd_total(pd_own_c, pd_c, pdc_recv, x, n_cols)
    inverse = 1.0 / jnp.sqrt(column_of(pivot_diag[0:1, :]))
    total_sq = jnp.zeros((1, rows_here), jnp.float32)
    per_t = max(LANES // m_rows, 1)
    for m in range(m_chunks):
        if m == m_chunks - 1:
            for d in range(1, n_rows):
                other = lax.rem(z + d, n_rows)
                arrived(landed.at[other], ket_recv.at[other])
            for place in range(per_device):
                block = device * per_device + place
                source = jnp.int32(0)
                for band in range(n_rows):
                    owner = band * column_size + column
                    for slot in range(slot_count):
                        fits = (slot < counts_ref[owner]) & (targets_ref[slot, owner] == block)
                        source = jnp.where(fits, jnp.int32(band), source)
                next_ref[place * block_rows:(place + 1) * block_rows, :] = landed[source]
        total = mine[m]
        for c in range(1, n_cols):
            other = lax.rem(x + c, n_cols)
            arrived(col_in.at[m, other], col_recv.at[m, other])
            total = total + col_in[m, other]
        rows = slice(m * m_rows, (m + 1) * m_rows)
        for h in range(rows_here // LANES):
            cut = slice(h * LANES, (h + 1) * LANES)
            scaled_t[rows, cut] = (prev_t[rows, cut] - total[:, cut]) * inverse[rows, :]
        scaled = scaled_t[rows, :]
        total_sq = total_sq + jnp.sum(scaled * scaled, axis=0, keepdims=True)
        if (m + 1) % per_t == 0:
            done = slice((m + 1 - per_t) * m_rows, (m + 1) * m_rows)
            new_ref[:, done] = jnp.transpose(scaled_t[done, :]).astype(jnp.bfloat16)
    diag_out_ref[...] = diag_ref[...] - total_sq

    for c in pdz + pds + pdc:
        c.wait_send()
    for d in range(1, n_rows):
        ket_copy(d).wait_send()

    @pl.when(z < n_rows - 1)
    def _():
        for q in range(z_chunks):
            z_copy(own, from_l, zr_send, l_recv, q, 1).wait_send()

    @pl.when(z > 0)
    def _():
        for q in range(z_chunks):
            z_copy(own, from_r, zl_send, r_recv, q, -1).wait_send()

    for m in range(m_chunks):
        for d in range(1, n_sub):
            sub_copy(m, d).wait_send()
        for c in range(1, n_cols):
            col_copy(m, c).wait_send()


def body(mesh_sizes, vectors, previous, pivots, diagonal, ket_blocks, tags, targets, counts, norms):
    n_rows, n_cols, n_sub = mesh_sizes
    width, band_rows = vectors.shape
    rows_here, batch = previous.shape
    slot_count, block_rows, _ = ket_blocks.shape
    z_chunks, m_chunks, hop_lead = 8, 4, 3
    z_rows, m_rows = batch // z_chunks, batch // m_chunks
    f32, bf16, dma = jnp.float32, jnp.bfloat16, pltpu.SemaphoreType.DMA
    line = pltpu.VMEM((z_chunks, z_rows, width), bf16)
    small = pltpu.VMEM((8, batch), f32)
    scratch = [
        pltpu.VMEM(vectors.shape, bf16), pltpu.VMEM(previous.shape, bf16),
        pltpu.VMEM(ket_blocks.shape, bf16), pltpu.VMEM((batch, band_rows), bf16),
        line, line, line, line, line, line,
        pltpu.VMEM((batch, rows_here), f32),
        pltpu.VMEM((m_chunks, n_sub, n_cols, m_rows, rows_here), f32),
        pltpu.VMEM((m_chunks, n_sub, n_cols, m_rows, rows_here), f32),
        pltpu.VMEM((m_chunks, m_rows, rows_here), f32),
        pltpu.VMEM((m_chunks, n_cols, m_rows, rows_here), f32),
        pltpu.VMEM((m_chunks, n_cols, m_rows, rows_here), f32),
        pltpu.VMEM((batch, rows_here), f32),
        pltpu.VMEM((n_rows, block_rows, batch), bf16),
        pltpu.VMEM((n_rows, block_rows, batch), bf16),
        pltpu.VMEM((n_rows + 1, 8, batch), f32), pltpu.VMEM((n_sub, 8, batch), f32),
        pltpu.VMEM((n_cols, 8, batch), f32), small, small,
        dma((3,)), dma((z_chunks,)), dma((z_chunks,)), dma((z_chunks,)), dma((z_chunks,)),
        dma((m_chunks, n_sub)), dma((m_chunks, n_sub)),
        dma((m_chunks, n_cols)), dma((m_chunks, n_cols)),
        dma((n_rows,)), dma((n_rows,)), dma((n_rows,)), dma((n_rows,)),
        dma((n_sub,)), dma((n_sub,)), dma((n_cols,)), dma((n_cols,)),
    ]
    hbm = pl.BlockSpec(memory_space=pl.ANY)
    vmem = pl.BlockSpec(memory_space=pltpu.VMEM)
    smem = pl.BlockSpec(memory_space=pltpu.SMEM)
    new_vectors, diag_out, next_columns = pl.pallas_call(
        functools.partial(kernel, (n_rows, n_cols, n_sub, hop_lead)),
        out_shape=(
            pltpu.VMEM((rows_here, batch), bf16),
            pltpu.VMEM((1, rows_here), f32),
            pltpu.VMEM((rows_here, batch), bf16),
        ),
        in_specs=[hbm, hbm, vmem, vmem, hbm, vmem, smem, smem, smem],
        out_specs=(vmem, vmem, vmem),
        scratch_shapes=scratch,
        compiler_params=pltpu.CompilerParams(
            collective_id=0, has_side_effects=True, vmem_limit_bytes=63 * 1024 * 1024),
    )(
        vectors, previous, pivots.reshape(1, batch), diagonal.reshape(1, rows_here),
        ket_blocks, tags, targets.T, counts, norms,
    )
    return new_vectors, diag_out.reshape(rows_here), next_columns


def solution(mesh):
    sizes = tuple(mesh.shape[name] for name in ("rows", "cols", "sub"))
    return jax.shard_map(
        functools.partial(body, sizes),
        mesh=mesh,
        in_specs=(
            P(("cols", "sub"), ("groups", "rows")),
            P(("groups", "rows", "cols", "sub"), None),
            P("groups"),
            P(("groups", "rows", "cols", "sub")),
            P(("groups", "rows", "cols", "sub"), None, None),
            P(("groups", "rows", "cols", "sub"), None),
            P("groups", None),
            P("groups"),
            P(),
        ),
        out_specs=(
            P(("groups", "rows", "cols", "sub"), None),
            P(("groups", "rows", "cols", "sub")),
            P(("groups", "rows", "cols", "sub"), None),
        ),
        check_vma=False,
    )
```
